32 devices in a mesh: src: 8 (over z, core), tgt: 4 (over y, x).
Axes of the slice: x: 2, y: 2, z: 4, core: 2. Of those that a mesh axis runs over, the one named last changes fastest.
Arguments:
- sources: float32 [64, 128, 4096], P(None, None, ('src', 'tgt')), may hold values from -6 to 6
- source_interp: float32 [128, 32, 4096], P(None, None, ('src', 'tgt')), may hold values from -0.5 to 0.5
- target_interp: float32 [128, 32, 4096], P(None, None, ('src', 'tgt')), may hold values from -1 to 1
- transfer: float32 [7, 32, 64, 4096], P(None, None, None, ('src', 'tgt')), may hold values from -0.75 to 0.75
Outputs:
- targets: float32 [64, 128, 4096], P(None, None, ('src', 'tgt'))
The draws below stay inside these ranges and needn't reach their ends.
All inputs are finite; a program needn't handle non-finite values.
Results may differ from the reference program's by a relative error of at most 0.00017.
Values sent between devices are 32-bit elements; how exact they have to be, the bound alone decides.
A program may use at most 128 MiB of HBM per device.

```python
import jax
import jax.numpy as jnp
from jax import lax

K = 32
R = 64
B = 128
LOCAL_LEVELS = 2
LEVELS = 7
NB = 4096
N_SRC = 8
N_TGT = 4


def shard_levels(rng, shape, cuts, least, top_value):
    def one(dim, parts):
        steps = jax.random.uniform(jax.random.fold_in(jax.random.fold_in(rng, 6), dim), (parts,), jnp.float32, least / len(cuts), top_value / len(cuts))
        return jnp.repeat(jnp.exp(steps), shape[dim] // parts).reshape((-1,) + (1,) * (len(shape) - dim - 1))

    level = one(*cuts[0])
    for cut in cuts[1:]:
        level = level * one(*cut)
    return level


def noise(key, shape, deviation, reach, cuts=(), held_as=jnp.bfloat16):
    drawn = deviation * jax.random.normal(key, shape, jnp.float32)
    if cuts:
        drawn = drawn * shard_levels(key, shape, cuts, -0.22, 0.18)
    return jnp.clip(drawn, -reach, reach).astype(held_as)


def setup_inputs(seed: int = 0) -> dict:
    keys = jax.random.split(jax.random.key(seed), 5)
    return {
        "sources": noise(keys[0], (R, B, NB), 1.0, 6.0, ((2, 32),), jnp.float32),
        "source_interp": noise(keys[1], (B, K, NB), B ** -0.5, 0.5, ((2, 32),), jnp.float32),
        "target_interp": noise(keys[2], (B, K, NB), K ** -0.5, 1.0, ((2, 32),), jnp.float32),
        "transfer": noise(keys[3], (LEVELS, K, 2 * K, NB), (2 * K) ** -0.5, 0.75, ((3, 32),), jnp.float32),
    }


def flip_axis(values, axis, half):
    shape = values.shape
    length = shape[axis]
    split = shape[:axis] + (length // (2 * half), 2, half) + shape[axis + 1:]
    return jnp.flip(values.reshape(split), axis + 1).reshape(shape)


def mixing(weight, coeffs):
    return jnp.einsum('kjg,jrg->krg', weight, coeffs, precision=lax.Precision.HIGHEST)


def reference(sources, source_interp, target_interp, transfer):
    rank = source_interp.shape[1]
    blocks_dev = sources.shape[2] // (N_SRC * N_TGT)
    local_bits = blocks_dev.bit_length() - 1
    src_bits = N_SRC.bit_length() - 1
    tgt_bits = N_TGT.bit_length() - 1
    order = [m for m in range(LOCAL_LEVELS)]
    order = order + [local_bits + tgt_bits + j for j in range(src_bits)]
    order = order + [local_bits + j for j in range(tgt_bits)]
    coeffs = jnp.einsum('bkg,rbg->krg', source_interp, sources, precision=lax.Precision.HIGHEST)
    for position, bit_pos in enumerate(order):
        weight = transfer[position]
        partner = flip_axis(coeffs, 2, 1 << bit_pos)
        coeffs = mixing(weight[:, :rank], coeffs) + mixing(weight[:, rank:], partner)
    return jnp.einsum('bkg,krg->rbg', target_interp, coeffs, precision=lax.Precision.HIGHEST)
```

```python
import functools

import jax
import jax.numpy as jnp
from jax import lax
from jax.experimental import pallas as pl
from jax.experimental.pallas import tpu as pltpu
from jax.sharding import PartitionSpec as P

ROWS = 8
TILES = 2
PAD = 8


def flip_mask(axis, bit):
    me = lax.axis_index(axis)
    half = 2**bit
    return me + half - 2 * half * ((me // half) % 2)


def mix(weight_at, source_at, store, depth, outs, tiles, block, unroll):
    def one_block(start):
        def step(outer, acc):
            acc = list(acc)
            for inner in range(unroll):
                j = outer * unroll + inner
                rows = [source_at(j, t) for t in range(tiles)]
                for i in range(block):
                    w = weight_at(start + i, j)
                    for t in range(tiles):
                        acc[i * tiles + t] = acc[i * tiles + t] + w * rows[t]
            return tuple(acc)

        zero = jnp.zeros((ROWS, 128), jnp.float32)
        acc = lax.fori_loop(0, depth // unroll, step, (zero,) * (block * tiles))
        for i in range(block):
            for t in range(tiles):
                store(start + i, t, acc[i * tiles + t])

    def body(b, carry):
        one_block(b * block)
        return carry

    lax.fori_loop(0, outs // block, body, 0)


def kernel(dims, sources, interp_in, interp_out, transfer, out,
           s_buf, si_buf, ti_buf, w_buf, c_buf, p_buf, o_buf,
           load_sem, s_sem, w_sem, o_sem, send_sem, recv_sem):
    rank, rhs, points, levels, local, partners = dims
    tiles = TILES
    width = ROWS * tiles
    chunks = rhs // width
    pitch = points + PAD

    loads_si = pltpu.make_async_copy(interp_in, si_buf, load_sem.at[0])
    loads_ti = pltpu.make_async_copy(interp_out, ti_buf, load_sem.at[1])

    def source_copy(r):
        return pltpu.make_async_copy(
            sources.at[r], s_buf.at[pl.ds(r * pitch, points)], s_sem.at[r])

    def weight_copy(n):
        return pltpu.make_async_copy(
            transfer.at[pl.ds(n * rank * 2 * rank, rank * 2 * rank)], w_buf.at[n], w_sem.at[n])

    def start_sources(r, carry):
        source_copy(r).start()
        return carry

    def wait_sources(r, carry):
        source_copy(r).wait()
        return carry

    loads_si.start()
    lax.fori_loop(0, rhs, start_sources, 0)
    for n in range(levels):
        weight_copy(n).start()
    loads_ti.start()

    barrier = pltpu.get_barrier_semaphore()
    where = [{axis: flip_mask(axis, bit)} for axis, bit in partners]
    for device in where:
        pl.semaphore_signal(barrier, inc=1, device_id=device, device_id_type=pl.DeviceIdType.MESH)
    pl.semaphore_wait(barrier, len(where))

    lane = lax.broadcasted_iota(jnp.int32, (ROWS, 128), 1)

    def at_chunk(c, k, t):
        return pl.ds(c * rank * width + k * width + t * ROWS, ROWS)

    def exchange(n, c):
        e = n - local
        part = pl.ds(c * rank * width, rank * width)
        return pltpu.make_async_remote_copy(
            src_ref=c_buf.at[n, part], dst_ref=p_buf.at[n, part],
            send_sem=send_sem.at[e, c], recv_sem=recv_sem.at[e, c],
            device_id=where[e], device_id_type=pl.DeviceIdType.MESH)

    def deliver(n, c):
        if n >= local:
            if n < levels:
                exchange(n, c).start()
            return
        half = 2**n

        def flip(k, carry):
            for t in range(tiles):
                x = c_buf[n, at_chunk(c, k, t), :]
                low = (lane // half) % 2 == 0
                p_buf[n, at_chunk(c, k, t), :] = jnp.where(
                    low, pltpu.roll(x, 128 - half, 1), pltpu.roll(x, half, 1))
            return carry

        lax.fori_loop(0, rank, flip, 0)

    def first(c):
        if c == 0:
            loads_si.wait()
        lax.fori_loop(c * width, (c + 1) * width, wait_sources, 0)

        def weight_at(k, b):
            return si_buf[pl.ds(b * rank + k, ROWS, stride=0), :]

        def source_at(b, t):
            return s_buf[pl.ds((c * width + t * ROWS) * pitch + b, ROWS, stride=pitch), :]

        def store(k, t, value):
            c_buf[0, at_chunk(c, k, t), :] = value

        mix(weight_at, source_at, store, points, rank, tiles, 32 // tiles, 4)
        deliver(0, c)

    def level(n, c):
        if c == 0:
            weight_copy(n).wait()
        if n >= local:
            exchange(n, c).wait_recv()
        block = 32 // tiles

        def body(b, carry):
            def step(outer, acc):
                acc = list(acc)
                for buf, base in ((c_buf, 0), (p_buf, rank)):
                    for inner in range(2):
                        j = outer * 2 + inner
                        rows = [buf[n, at_chunk(c, j, t), :] for t in range(tiles)]
                        for i in range(block):
                            w = w_buf[n, pl.ds((b * block + i) * 2 * rank + base + j, ROWS, stride=0), :]
                            for t in range(tiles):
                                acc[i * tiles + t] = acc[i * tiles + t] + w * rows[t]
                return tuple(acc)

            zero = jnp.zeros((ROWS, 128), jnp.float32)
            acc = lax.fori_loop(0, rank // 2, step, (zero,) * (block * tiles))
            for i in range(block):
                for t in range(tiles):
                    c_buf[n + 1, at_chunk(c, b * block + i, t), :] = acc[i * tiles + t]
            return carry

        lax.fori_loop(0, rank // block, body, 0)
        deliver(n + 1, c)

    def out_copy(r):
        return pltpu.make_async_copy(
            o_buf.at[pl.ds(r * pitch, points)], out.at[r], o_sem.at[r])

    def start_out(r, carry):
        out_copy(r).start()
        return carry

    def wait_out(r, carry):
        out_copy(r).wait()
        return carry

    def last(c):
        if c == 0:
            loads_ti.wait()

        def weight_at(b, k):
            return ti_buf[pl.ds(b * rank + k, ROWS, stride=0), :]

        def source_at(k, t):
            return c_buf[levels, at_chunk(c, k, t), :]

        def store(b, t, value):
            o_buf[pl.ds((c * width + t * ROWS) * pitch + b, ROWS, stride=pitch), :] = value

        mix(weight_at, source_at, store, rank, points, tiles, 32 // tiles, 4)
        lax.fori_loop(c * width, (c + 1) * width, start_out, 0)

    for task, c in schedule(chunks, levels, local, partners):
        if task == 0:
            first(c)
        elif task <= levels:
            level(task - 1, c)
        else:
            last(c)

    for n in range(local, levels):
        for c in range(chunks):
            exchange(n, c).wait_send()
    lax.fori_loop(0, rhs, wait_out, 0)


def schedule(chunks, levels, local, partners):
    work = [2.0] + [1.0] * levels + [2.0]
    flight = [0.0] * (levels + 2)
    links = [None] * (levels + 2)
    for e, (axis, bit) in enumerate(partners):
        flight[local + e + 1] = 0.5 if (axis == "src" and bit == 0) else 5.0
        links[local + e + 1] = (axis, bit) if axis == "tgt" or bit == 0 else axis
    busy, ready, nxt = {}, {(0, c): 0.0 for c in range(chunks)}, {c: 0 for c in range(chunks)}
    now, order = 0.0, []
    while nxt:
        open_now = [(c, t) for c, t in nxt.items() if ready[t, c] <= now]
        if not open_now:
            now = min(ready[t, c] for c, t in nxt.items())
            continue
        c, t = min(open_now)
        now += work[t]
        order.append((t, c))
        if t == levels + 1:
            del nxt[c]
            continue
        start = now
        if links[t + 1] is not None:
            start = max(now, busy.get(links[t + 1], 0.0))
            busy[links[t + 1]] = start + flight[t + 1]
        ready[t + 1, c] = start + flight[t + 1] + (0.0 if links[t + 1] is None else 1.5)
        nxt[c] = t + 1
    return order


def body(sources, source_interp, target_interp, transfer):
    rhs, points, blocks = sources.shape
    rank = source_interp.shape[1]
    levels = transfer.shape[0]
    src_bits = lax.axis_size("src").bit_length() - 1
    tgt_bits = lax.axis_size("tgt").bit_length() - 1
    local = levels - src_bits - tgt_bits
    partners = [("src", b) for b in range(src_bits)] + [("tgt", b) for b in range(tgt_bits)]
    dims = (rank, rhs, points, levels, local, partners)
    chunks = rhs // (ROWS * TILES)
    pitch = points + PAD
    f32 = jnp.float32
    any_space = pl.BlockSpec(memory_space=pl.ANY)
    return pl.pallas_call(
        functools.partial(kernel, dims),
        out_shape=jax.ShapeDtypeStruct(sources.shape, f32),
        in_specs=[any_space] * 4,
        out_specs=any_space,
        scratch_shapes=[
            pltpu.VMEM((rhs * pitch, blocks), f32),
            pltpu.VMEM((points * rank, blocks), f32),
            pltpu.VMEM((points * rank, blocks), f32),
            pltpu.VMEM((levels, rank * 2 * rank, blocks), f32),
            pltpu.VMEM((levels + 1, rhs * rank, blocks), f32),
            pltpu.VMEM((levels, rhs * rank, blocks), f32),
            pltpu.VMEM((rhs * pitch, blocks), f32),
            pltpu.SemaphoreType.DMA((2,)),
            pltpu.SemaphoreType.DMA((rhs,)),
            pltpu.SemaphoreType.DMA((levels,)),
            pltpu.SemaphoreType.DMA((rhs,)),
            pltpu.SemaphoreType.DMA((len(partners), chunks)),
            pltpu.SemaphoreType.DMA((len(partners), chunks)),
        ],
        compiler_params=pltpu.CompilerParams(
            collective_id=0, has_side_effects=True, vmem_limit_bytes=60 * 2**20),
    )(sources, source_interp.reshape(points * rank, blocks),
      target_interp.reshape(points * rank, blocks),
      transfer.reshape(levels * rank * 2 * rank, blocks))


def solution(mesh):
    placed = (
        P(None, None, ("src", "tgt")),
        P(None, None, ("src", "tgt")),
        P(None, None, ("src", "tgt")),
        P(None, None, None, ("src", "tgt")),
    )
    return jax.shard_map(
        body, mesh=mesh, in_specs=placed, out_specs=P(None, None, ("src", "tgt")), check_vma=False
    )
```

```python
import functools

import jax
import jax.numpy as jnp
from jax import lax
from jax.experimental import pallas as pl
from jax.experimental.pallas import tpu as pltpu
from jax.sharding import PartitionSpec as P

ROWS = 8
TILES = 2
PAD = 8


def flip_mask(axis, bit):
    me = lax.axis_index(axis)
    half = 2**bit
    return me + half - 2 * half * ((me // half) % 2)


def mix(weight_at, source_at, store, depth, outs, tiles, block, unroll):
    def one_block(start):
        def step(outer, acc):
            acc = list(acc)
            for inner in range(unroll):
                j = outer * unroll + inner
                rows = [source_at(j, t) for t in range(tiles)]
                for i in range(block):
                    w = weight_at(start + i, j)
                    for t in range(tiles):
                        acc[i * tiles + t] = acc[i * tiles + t] + w * rows[t]
            return tuple(acc)

        zero = jnp.zeros((ROWS, 128), jnp.float32)
        acc = lax.fori_loop(0, depth // unroll, step, (zero,) * (block * tiles))
        for i in range(block):
            for t in range(tiles):
                store(start + i, t, acc[i * tiles + t])

    def body(b, carry):
        one_block(b * block)
        return carry

    lax.fori_loop(0, outs // block, body, 0)


def kernel(dims, sources, interp_in, interp_out, transfer, out,
           s_buf, si_buf, ti_buf, w_buf, c_buf, p_buf, o_buf,
           load_sem, s_sem, w_sem, o_sem, send_sem, recv_sem):
    rank, rhs, points, levels, local, partners = dims
    tiles = TILES
    width = ROWS * tiles
    chunks = rhs // width
    pitch = points + PAD

    loads_si = pltpu.make_async_copy(interp_in, si_buf, load_sem.at[0])
    loads_ti = pltpu.make_async_copy(interp_out, ti_buf, load_sem.at[1])

    def source_copy(r):
        return pltpu.make_async_copy(
            sources.at[r], s_buf.at[pl.ds(r * pitch, points)], s_sem.at[r])

    def weight_copy(n):
        return pltpu.make_async_copy(
            transfer.at[pl.ds(n * rank * 2 * rank, rank * 2 * rank)], w_buf.at[n], w_sem.at[n])

    def start_sources(r, carry):
        source_copy(r).start()
        return carry

    def wait_sources(r, carry):
        source_copy(r).wait()
        return carry

    loads_si.start()
    lax.fori_loop(0, rhs, start_sources, 0)
    for n in range(levels):
        weight_copy(n).start()
    loads_ti.start()

    barrier = pltpu.get_barrier_semaphore()
    where = [{axis: flip_mask(axis, bit)} for axis, bit in partners]
    for device in where:
        pl.semaphore_signal(barrier, inc=1, device_id=device, device_id_type=pl.DeviceIdType.MESH)
    pl.semaphore_wait(barrier, len(where))

    lane = lax.broadcasted_iota(jnp.int32, (ROWS, 128), 1)

    def at_chunk(c, k, t):
        return pl.ds(c * rank * width + k * width + t * ROWS, ROWS)

    def exchange(n, c):
        e = n - local
        part = pl.ds(c * rank * width, rank * width)
        return pltpu.make_async_remote_copy(
            src_ref=c_buf.at[n, part], dst_ref=p_buf.at[n, part],
            send_sem=send_sem.at[e, c], recv_sem=recv_sem.at[e, c],
            device_id=where[e], device_id_type=pl.DeviceIdType.MESH)

    def deliver(n, c):
        if n >= local:
            if n < levels:
                exchange(n, c).start()
            return
        half = 2**n

        low = (lane // half) % 2 == 0
        group = 8

        def flip(outer, carry):
            places = [at_chunk(c, outer * group + i, t) for i in range(group) for t in range(tiles)]
            values = [c_buf[n, place, :] for place in places]
            ahead = [pltpu.roll(x, 128 - half, 1) for x in values]
            behind = [pltpu.roll(x, half, 1) for x in values]
            for place, up, down in zip(places, ahead, behind):
                p_buf[n, place, :] = jnp.where(low, up, down)
            return carry

        lax.fori_loop(0, rank // group, flip, 0)

    def first(c):
        if c == 0:
            loads_si.wait()
        lax.fori_loop(c * width, (c + 1) * width, wait_sources, 0)

        def weight_at(k, b):
            return si_buf[pl.ds(b * rank + k, ROWS, stride=0), :]

        def source_at(b, t):
            return s_buf[pl.ds((c * width + t * ROWS) * pitch + b, ROWS, stride=pitch), :]

        def store(k, t, value):
            c_buf[0, at_chunk(c, k, t), :] = value

        mix(weight_at, source_at, store, points, rank, tiles, 32 // tiles, 4)
        deliver(0, c)

    def level(n, c):
        if c == 0:
            weight_copy(n).wait()
        if n >= local:
            exchange(n, c).wait_recv()
        block = 32 // tiles

        def body(b, carry):
            def step(outer, acc):
                acc = list(acc)
                for buf, base in ((c_buf, 0), (p_buf, rank)):
                    for inner in range(2):
                        j = outer * 2 + inner
                        rows = [buf[n, at_chunk(c, j, t), :] for t in range(tiles)]
                        for i in range(block):
                            w = w_buf[n, pl.ds((b * block + i) * 2 * rank + base + j, ROWS, stride=0), :]
                            for t in range(tiles):
                                acc[i * tiles + t] = acc[i * tiles + t] + w * rows[t]
                return tuple(acc)

            zero = jnp.zeros((ROWS, 128), jnp.float32)
            acc = lax.fori_loop(0, rank // 2, step, (zero,) * (block * tiles))
            for i in range(block):
                for t in range(tiles):
                    c_buf[n + 1, at_chunk(c, b * block + i, t), :] = acc[i * tiles + t]
            return carry

        lax.fori_loop(0, rank // block, body, 0)
        deliver(n + 1, c)

    def out_copy(r):
        return pltpu.make_async_copy(
            o_buf.at[pl.ds(r * pitch, points)], out.at[r], o_sem.at[r])

    def start_out(r, carry):
        out_copy(r).start()
        return carry

    def wait_out(r, carry):
        out_copy(r).wait()
        return carry

    def last(c):
        if c == 0:
            loads_ti.wait()

        def weight_at(b, k):
            return ti_buf[pl.ds(b * rank + k, ROWS, stride=0), :]

        def source_at(k, t):
            return c_buf[levels, at_chunk(c, k, t), :]

        def store(b, t, value):
            o_buf[pl.ds((c * width + t * ROWS) * pitch + b, ROWS, stride=pitch), :] = value

        mix(weight_at, source_at, store, rank, points, tiles, 32 // tiles, 4)
        lax.fori_loop(c * width, (c + 1) * width, start_out, 0)

    for task, c in schedule(chunks, levels, local, partners):
        if task == 0:
            first(c)
        elif task <= levels:
            level(task - 1, c)
        else:
            last(c)

    for n in range(local, levels):
        for c in range(chunks):
            exchange(n, c).wait_send()
    lax.fori_loop(0, rhs, wait_out, 0)


def schedule(chunks, levels, local, partners):
    work = [2.0] + [1.0] * levels + [2.0]
    flight = [0.0] * (levels + 2)
    links = [None] * (levels + 2)
    for e, (axis, bit) in enumerate(partners):
        flight[local + e + 1] = 0.5 if (axis == "src" and bit == 0) else 4.5
        links[local + e + 1] = (axis, bit) if axis == "tgt" or bit == 0 else axis
    busy, ready, nxt = {}, {(0, c): 0.0 for c in range(chunks)}, {c: 0 for c in range(chunks)}
    now, order = 0.0, []
    while nxt:
        open_now = [(c, t) for c, t in nxt.items() if ready[t, c] <= now]
        if not open_now:
            now = min(ready[t, c] for c, t in nxt.items())
            continue
        c, t = min(open_now)
        now += work[t]
        order.append((t, c))
        if t == levels + 1:
            del nxt[c]
            continue
        start = now
        if links[t + 1] is not None:
            start = max(now, busy.get(links[t + 1], 0.0))
            busy[links[t + 1]] = start + flight[t + 1]
        ready[t + 1, c] = start + flight[t + 1] + (0.0 if links[t + 1] is None else 1.5)
        nxt[c] = t + 1
    return order


def body(sources, source_interp, target_interp, transfer):
    rhs, points, blocks = sources.shape
    rank = source_interp.shape[1]
    levels = transfer.shape[0]
    src_bits = lax.axis_size("src").bit_length() - 1
    tgt_bits = lax.axis_size("tgt").bit_length() - 1
    local = levels - src_bits - tgt_bits
    partners = [("src", b) for b in range(src_bits)] + [("tgt", b) for b in range(tgt_bits)]
    dims = (rank, rhs, points, levels, local, partners)
    chunks = rhs // (ROWS * TILES)
    pitch = points + PAD
    f32 = jnp.float32
    any_space = pl.BlockSpec(memory_space=pl.ANY)
    return pl.pallas_call(
        functools.partial(kernel, dims),
        out_shape=jax.ShapeDtypeStruct(sources.shape, f32),
        in_specs=[any_space] * 4,
        out_specs=any_space,
        scratch_shapes=[
            pltpu.VMEM((rhs * pitch, blocks), f32),
            pltpu.VMEM((points * rank, blocks), f32),
            pltpu.VMEM((points * rank, blocks), f32),
            pltpu.VMEM((levels, rank * 2 * rank, blocks), f32),
            pltpu.VMEM((levels + 1, rhs * rank, blocks), f32),
            pltpu.VMEM((levels, rhs * rank, blocks), f32),
            pltpu.VMEM((rhs * pitch, blocks), f32),
            pltpu.SemaphoreType.DMA((2,)),
            pltpu.SemaphoreType.DMA((rhs,)),
            pltpu.SemaphoreType.DMA((levels,)),
            pltpu.SemaphoreType.DMA((rhs,)),
            pltpu.SemaphoreType.DMA((len(partners), chunks)),
            pltpu.SemaphoreType.DMA((len(partners), chunks)),
        ],
        compiler_params=pltpu.CompilerParams(
            collective_id=0, has_side_effects=True, vmem_limit_bytes=60 * 2**20),
    )(sources, source_interp.reshape(points * rank, blocks),
      target_interp.reshape(points * rank, blocks),
      transfer.reshape(levels * rank * 2 * rank, blocks))


def solution(mesh):
    placed = (
        P(None, None, ("src", "tgt")),
        P(None, None, ("src", "tgt")),
        P(None, None, ("src", "tgt")),
        P(None, None, None, ("src", "tgt")),
    )
    return jax.shard_map(
        body, mesh=mesh, in_specs=placed, out_specs=P(None, None, ("src", "tgt")), check_vma=False
    )
```
